768 devices in a mesh: grp: 24 (over y_lo, z), tp: 32 (over x, y_hi, core).
Axes of the slice: x: 4, y: 8 (y_hi: 4, y_lo: 2; y = y_hi * 2 + y_lo), z: 12, core: 2. Of those that a mesh axis runs over, the one named last changes fastest.
Arguments:
- hidden: bfloat16 [6144, 8192], P('grp'), may hold values from -30 to 30
- proj_weight: bfloat16 [8192, 8192], P(None, 'tp'), may hold values from -0.32040776 to 0.32040776
- proj_bias: float32 [8192], P('tp'), may hold values from -3 to 3
- tile_pos: int32 [768], replicated, may hold values from 0 to 2303, as said below
- text_embed: bfloat16 [18432, 8192], P('grp', 'tp'), may hold values from -76 to 76
- norm_gain: float32 [8192], P('tp'), may hold values from 0.25 to 1.75
- d_normed: bfloat16 [18432, 8192], P('grp', 'tp'), may hold values from -6 to 6
Outputs:
- normed: bfloat16 [18432, 8192], P('grp', 'tp')
- d_text: bfloat16 [18432, 8192], P('grp', 'tp')
- d_hidden: bfloat16 [6144, 8192], P('grp', 'tp')
The draws below stay inside these ranges and needn't reach their ends.
Inputs may be any that keep to these rules, and one draw needn't show every extreme that they name: `tile_pos`: all positions are distinct. Of the tiles k * 32 to (k + 1) * 32 - 1, at most 2 lie in the 96 tile positions of one index of grp, and in every draw each such block has exactly 2 tiles in some index of grp.
All inputs are finite; a program needn't handle non-finite values.
Results may differ from the reference program's by a relative error of at most 0.015.
Values may be sent and summed in bfloat16 or wider, within the bound.
No kernel may reach another device: no remote copies, remote signals or barrier semaphores. Data moves between devices by JAX's collectives and lax.ppermute only.
A program may use at most 64 MiB of HBM per device.

```python
import math
import jax
import jax.numpy as jnp
from jax import lax

D = 8192
TILE = 8
TILES_DEV = 32
TPD = 96
CAP = 2
NTILE = 768
IMG_ROWS = 6144
TOKENS = 18432
N_GRP = 24
N_TP = 32


def col_profile(key_cols, span_width):
    rising = 10.0 ** (jnp.arange(span_width, dtype=jnp.float32) / span_width - 0.5)
    jitter = jnp.exp(jax.random.uniform(key_cols, (span_width,), jnp.float32, -0.4, 0.4))
    return rising * jitter


def row_profile(key_rows, count_rows, lowest, highest):
    return jnp.exp(jax.random.uniform(key_rows, (count_rows, 1), jnp.float32, math.log(lowest), math.log(highest)))


def draw_hidden(key, part):
    key_rows, key_cols, key_vals = jax.random.split(jax.random.fold_in(key, 11), 3)
    scales = row_profile(key_rows, IMG_ROWS, 0.5, 5.0)
    entries = jnp.clip(jax.random.normal(key_vals, (IMG_ROWS, D), jnp.float32), -4.0, 4.0)
    jitter = jnp.exp(jax.random.uniform(key_cols, (1, D), jnp.float32, -0.4, 0.4))
    return (entries * scales * jitter).astype(jnp.bfloat16)


def draw_proj_weight(key, part):
    key_cols, key_vals = jax.random.split(jax.random.fold_in(key, 23), 2)
    scales = col_profile(key_cols, D)[None, :] / math.sqrt(D)
    entries = jnp.clip(jax.random.normal(key_vals, (D, D), jnp.float32), -4.0, 4.0)
    return (entries * scales).astype(jnp.bfloat16)


def draw_text_embed(key, part):
    key_rows, key_cols, key_vals = jax.random.split(jax.random.fold_in(key, 37), 3)
    scales = row_profile(key_rows, TOKENS, 0.3, 3.0)
    columns = col_profile(key_cols, D)[None, :]
    entries = jnp.clip(jax.random.normal(key_vals, (TOKENS, D), jnp.float32), -4.0, 4.0)
    return (entries * scales * columns).astype(jnp.bfloat16)


def draw_tile_pos(key, part):
    key_offsets, key_starts = jax.random.split(jax.random.fold_in(key, 53), 2)
    fanout = TILES_DEV // CAP
    offsets = jax.random.permutation(key_offsets, N_GRP).astype(jnp.int32)[:fanout]
    starts = jax.random.randint(key_starts, (N_GRP,), 0, TPD - TILES_DEV + 1, dtype=jnp.int32)
    tile_index = jnp.arange(NTILE, dtype=jnp.int32)
    source = tile_index // TILES_DEV
    within = tile_index % TILES_DEV
    target = (source + offsets[within // CAP]) % N_GRP
    return (target * TPD + starts[target] + within).astype(jnp.int32)


def block_levels(stream_key, dims, pieces, least, high):
    loudness, own = 1.0, jax.random.fold_in(stream_key, 6)
    for position, blocks in pieces:
        draws = jnp.exp(jax.random.uniform(jax.random.fold_in(own, position), (blocks,), jnp.float32, least / len(pieces), high / len(pieces)))
        loudness = loudness * jnp.repeat(draws, dims[position] // blocks).reshape([-1 if axis == position else 1 for axis in range(len(dims))])
    return loudness


def centred(own_key, dims, deviation, limit, shards=(), kind=jnp.bfloat16):
    values = deviation * jax.random.normal(own_key, dims, jnp.float32)
    if shards:
        values = values * block_levels(own_key, dims, shards, -0.22, 0.18)
    return jnp.clip(values, -limit, limit).astype(kind)


def setup_inputs(seed: int = 0) -> dict:
    key_list = jax.random.split(jax.random.key(seed), 8)
    hidden = draw_hidden(jax.random.fold_in(key_list[7], 71), 0)
    proj_weight = draw_proj_weight(jax.random.fold_in(key_list[7], 71), 0)
    proj_bias = centred(key_list[2], (D,), 0.5, 3.0, ((0, 32),), jnp.float32)
    tile_pos = draw_tile_pos(jax.random.fold_in(key_list[7], 71), 0)
    text_embed = draw_text_embed(jax.random.fold_in(key_list[7], 71), 0)
    norm_gain = jnp.clip(1.0 + 0.15 * jax.random.normal(key_list[5], (D,), jnp.float32), 0.25, 1.75)
    d_normed = centred(key_list[6], (TOKENS, D), 1.0, 6.0, ((0, 24), (1, 32)))
    return {"hidden": hidden, "proj_weight": proj_weight, "proj_bias": proj_bias, "tile_pos": tile_pos, "text_embed": text_embed, "norm_gain": norm_gain, "d_normed": d_normed}


epsilon = 1e-05

def gelu_slope(values):
    normal_cdf = 0.5 * (1.0 + lax.erf(values * 0.7071067811865476))
    density = jnp.exp(-0.5 * values * values) * 0.3989422804014327
    return normal_cdf + values * density

def reference(hidden, proj_weight, proj_bias, tile_pos, text_embed, norm_gain, d_normed):
    hidden_wide = hidden.astype(jnp.float32)
    activated = jax.nn.gelu(hidden_wide, approximate=False).astype(jnp.bfloat16)
    image_rows = (jnp.dot(activated, proj_weight, preferred_element_type=jnp.float32) + proj_bias).astype(jnp.bfloat16)
    document = text_embed.reshape(TOKENS // TILE, TILE * D)
    merged = document.at[tile_pos].set(image_rows.reshape(NTILE, TILE * D)).reshape(TOKENS, D)
    is_image = jnp.zeros((TOKENS // TILE,), jnp.float32).at[tile_pos].set(1.0)
    wide_merged = merged.astype(jnp.float32)
    inverse = lax.rsqrt(lax.optimization_barrier(jnp.mean(wide_merged * wide_merged, axis=1, keepdims=True)) + epsilon)
    normed = (wide_merged * inverse * norm_gain).astype(jnp.bfloat16)
    grad_in = d_normed.astype(jnp.float32) * norm_gain
    cross_mean = lax.optimization_barrier(jnp.mean(grad_in * wide_merged, axis=1, keepdims=True))
    d_merged = inverse * (grad_in - wide_merged * inverse * inverse * cross_mean)
    d_tiles = d_merged.reshape(TOKENS // TILE, TILE * D)
    d_text = jnp.where(is_image[:, None] > 0.5, 0.0, d_tiles).astype(jnp.bfloat16).reshape(TOKENS, D)
    d_image = d_tiles[tile_pos].astype(jnp.bfloat16).reshape(IMG_ROWS, D)
    blocks = D // N_TP

    def add_block(running, block_index):
        columns = lax.dynamic_slice_in_dim(d_image, block_index * blocks, blocks, 1)
        weights = lax.dynamic_slice_in_dim(proj_weight, block_index * blocks, blocks, 1)
        partial_value = lax.dot_general(columns, weights, (((1,), (1,)), ((), ())), preferred_element_type=jnp.float32)
        partial_value = lax.optimization_barrier(partial_value.astype(jnp.bfloat16)).astype(jnp.float32)
        return (running + partial_value, None)
    d_act, _ = lax.scan(add_block, jnp.zeros((IMG_ROWS, D), jnp.float32), jnp.arange(N_TP, dtype=jnp.int32))
    d_hidden = (d_act * gelu_slope(hidden_wide)).astype(jnp.bfloat16)
    return (normed, d_text, d_hidden)
```

```python
import jax
import jax.numpy as jnp
from jax import lax
from jax.experimental import pallas as pl
from jax.experimental.pallas import tpu as pltpu
from jax.sharding import Mesh, PartitionSpec as P


TILE = 8
X, Y, C = 4, 4, 2
LANES = 128
GRANT = 16 << 20
LARGE_GRANT = 49 << 20

epsilon = 1e-05
bf16, f32 = jnp.bfloat16, jnp.float32


def gelu(values):
    return values * (0.5 * (1.0 + lax.erf(values * 0.7071067811865476)))


def gelu_slope(values):
    normal_cdf = 0.5 * (1.0 + lax.erf(values * 0.7071067811865476))
    density = jnp.exp(-0.5 * values * values) * 0.3989422804014327
    return normal_cdf + values * density


def match_table(wanted, choices_count):
    return wanted[None, :] == jnp.arange(choices_count, dtype=jnp.int32)[:, None]


def row_sums(image_rows, pair_rows, image_grad, pair_grad, text_embed, d_normed, norm_gain):
    rows, cols = image_rows.shape
    texts = text_embed.shape[0] // rows
    count = 2 + 2 * texts

    def kernel(image_r, pair_r, image_g, pair_g, text_r, d_r, gain_r, o_ref):
        lane = lax.broadcasted_iota(jnp.int32, (rows, LANES), 1)
        table = jnp.zeros((rows, LANES), f32)

        def put(table, index, values):
            return jnp.where(lane == index, jnp.sum(values, axis=1, keepdims=True), table)

        wide, pair = image_r[...].astype(f32), pair_r[...].astype(f32)
        table = put(table, 0, wide * wide + pair * pair)
        table = put(table, 1, image_g[...] * wide + pair_g[...] * pair)
        for i in range(texts):
            text = text_r[pl.ds(i * rows, rows), :].astype(f32)
            grad = d_r[pl.ds(i * rows, rows), :].astype(f32) * gain_r[...]
            table = put(table, 2 + i, text * text)
            table = put(table, 2 + texts + i, grad * text)
        flat = table.T[:count]
        o_ref[...] = jnp.broadcast_to(flat[None], (X * Y, count, rows))

    return pl.pallas_call(
        kernel,
        out_shape=jax.ShapeDtypeStruct((X * Y, count, rows), f32),
        compiler_params=pltpu.CompilerParams(vmem_limit_bytes=GRANT),
        cost_estimate=pl.CostEstimate(
            flops=8 * rows * cols * (texts + 2), bytes_accessed=4 * rows * cols * (texts + 3), transcendentals=0
        ),
    )(image_rows, pair_rows, image_grad, pair_grad, text_embed, d_normed, norm_gain)


def product(own_weight, pair_weight, sums, rows_pair, grads_pair, norm_gain, picks, core, width):
    features, cols = own_weight.shape[-2:]
    rows = rows_pair[0].shape[0]
    half = Y // 2
    groups, each = 4, 2
    steps = groups * each

    def kernel(pick, own_w, pair_w, sums_r, own_r, pair_r, own_g, pair_g, gain, *rest):
        normed, outs, own_d, pair_d = rest[0], rest[1:5], rest[5], rest[6]
        step = pl.program_id(0)

        @pl.when(step == 0)
        def _():
            total = jnp.sum(sums_r[...], axis=0)
            full = jnp.concatenate([total, jnp.zeros((LANES - total.shape[0], rows), f32)], axis=0)
            columns = full.T
            inverse = lax.rsqrt(columns[:, 0:1] / width + epsilon)
            cross_mean = columns[:, 1:2] / width

            def gradient(wide, grad):
                d_rows = inverse * (grad - wide * inverse * inverse * cross_mean)
                return d_rows.astype(bf16)

            wide = own_r[...].astype(f32)
            own_d[...] = gradient(wide, own_g[...])
            pair_d[...] = gradient(pair_r[...].astype(f32), pair_g[...])
            normed[...] = (wide * inverse * gain[...]).astype(bf16)

        def part(w, g):
            return lax.dot_general(
                w[...].reshape(half * features, cols),
                g[...],
                (((1,), (1,)), ((), ())),
                preferred_element_type=f32,
            )

        total = part(own_w, own_d) + part(pair_w, pair_d)
        total = total.astype(bf16).reshape(1, half, features, rows)
        for k, out in enumerate(outs):

            @pl.when(step // each == k)
            def _(out=out):
                out[...] = total

    def whole(*shape):
        return pl.BlockSpec(shape, lambda i, s: (0,) * len(shape))

    weight_spec = pl.BlockSpec(
        (None, half, None, features, cols), lambda i, s: (s[i], (i // each) % 2, s[steps], 0, 0)
    )

    def out_spec(k):
        return pl.BlockSpec(
            (1, half, features, rows), lambda i, s: (jnp.clip(i - each * k, 0, each - 1), 0, 0, 0)
        )

    return pl.pallas_call(
        kernel,
        grid_spec=pltpu.PrefetchScalarGridSpec(
            num_scalar_prefetch=1,
            grid=(steps,),
            in_specs=[weight_spec, weight_spec, whole(*sums.shape)]
            + [whole(rows, cols)] * 4
            + [whole(1, cols)],
            out_specs=[whole(rows, cols)] + [out_spec(k) for k in range(groups)],
            scratch_shapes=[pltpu.VMEM((rows, cols), bf16)] * 2,
        ),
        out_shape=[jax.ShapeDtypeStruct((rows, cols), bf16)]
        + [jax.ShapeDtypeStruct((each, half, features, rows), bf16)] * groups,
        compiler_params=pltpu.CompilerParams(vmem_limit_bytes=LARGE_GRANT),
        cost_estimate=pl.CostEstimate(
            flops=4 * steps * half * features * cols * rows,
            bytes_accessed=2 * steps * half * features * (2 * cols + rows),
            transcendentals=rows,
        ),
    )(jnp.stack([*picks, core]), own_weight, pair_weight, sums, *rows_pair, *grads_pair, norm_gain)


def combined(kept_a, got_a, last_a, kept_b, got_b, last_b):
    half, features, rows = last_a.shape

    def kernel(kept_a, got_a, last_a, kept_b, got_b, last_b, o_ref):
        for at, parts in ((0, (kept_a, got_a, last_a)), (half, (kept_b, got_b, last_b))):
            total = sum(part[...].astype(f32) for part in parts)
            o_ref[pl.ds(at, half)] = total.astype(bf16)

    second = pl.BlockSpec((None, half, features, rows), lambda i: (1, 0, 0, 0))
    whole = pl.BlockSpec((half, features, rows), lambda i: (0, 0, 0))
    return pl.pallas_call(
        kernel,
        grid=(1,),
        in_specs=[second, second, whole] * 2,
        out_specs=pl.BlockSpec((2 * half, features, rows), lambda i: (0, 0, 0)),
        out_shape=jax.ShapeDtypeStruct((2 * half, features, rows), bf16),
        compiler_params=pltpu.CompilerParams(vmem_limit_bytes=GRANT),
        cost_estimate=pl.CostEstimate(
            flops=4 * half * features * rows,
            bytes_accessed=16 * half * features * rows,
            transcendentals=0,
        ),
    )(kept_a, got_a, last_a, kept_b, got_b, last_b)


def swap_pair(value):
    return lax.ppermute(value, "core", [(0, 1), (1, 0)])


def swap_even(value):
    return lax.ppermute(value, "x", [(i, i ^ 1) for i in range(X)])


def swap_odd(value):
    return lax.ppermute(value, "x", [(i, 3 - i) for i in range(X)])


def swap_all(value, axis):
    return lax.all_to_all(value, axis, split_axis=0, concat_axis=0, tiled=True)


def on_device(hidden, proj_weight, proj_bias, tile_pos, text_embed, norm_gain, d_normed):
    rows_dev, model_width = hidden.shape
    local_cols = proj_weight.shape[1]
    tok_dev = text_embed.shape[0]
    groups = lax.axis_size("grp")
    group_index = lax.axis_index("grp")
    core = lax.axis_index("core")
    here = lax.axis_index("x")
    lane_index = (here * Y + lax.axis_index("y")) * C + core
    tiles_dev = rows_dev // TILE
    spread = tok_dev // TILE
    total_tiles = tiles_dev * groups
    capacity = max(2, (tiles_dev + groups - 1) // groups)
    slot_rows = groups * capacity * TILE

    target = tile_pos // spread
    local_pos = tile_pos - group_index * spread
    tile_index = jnp.arange(total_tiles, dtype=jnp.int32)
    source = tile_index // tiles_dev
    earlier = (
        (source[:, None] == source[None, :])
        & (target[:, None] == target[None, :])
        & (tile_index[:, None] < tile_index[None, :])
    )
    standing = jnp.sum(earlier.astype(jnp.int32), axis=0)

    def slots_of(names, rows, slot):
        row = jnp.arange(rows, dtype=jnp.int32)
        chosen = names[:, None] == (row // TILE)[None, :]
        found = slot[:, None] * TILE + (row % TILE)[None, :] + 1
        return jnp.sum(jnp.where(chosen, found, 0), axis=0) - 1

    doc_slot = slots_of(local_pos, tok_dev, source * capacity + standing)
    image_slot = slots_of(
        tile_index - group_index * tiles_dev, rows_dev, target * capacity + standing
    )
    receiver = match_table(doc_slot, slot_rows).astype(bf16)
    sender = match_table(image_slot, slot_rows).astype(bf16)

    def gathered(table, rows):
        return jnp.dot(table, rows, preferred_element_type=f32).astype(bf16)

    def scattered(table, rows):
        return lax.dot_general(table, rows, (((0,), (0,)), ((), ())), preferred_element_type=f32)

    def exchange(rows):
        split = rows.reshape(groups, capacity * TILE, local_cols)
        return swap_all(split, "grp").reshape(slot_rows, local_cols)

    fetch_out = gathered(receiver, d_normed)
    fetch_in = exchange(fetch_out)

    pair_weight = swap_pair(proj_weight)

    activated = gelu(hidden.astype(f32)).astype(bf16)
    image_rows = jnp.dot(activated, proj_weight, preferred_element_type=f32) + proj_bias
    image_rows = image_rows.astype(bf16)
    pair_rows = swap_pair(image_rows)

    late_sender, pair_rows = lax.optimization_barrier((sender, pair_rows))
    image_cot = scattered(late_sender, fetch_in).astype(bf16)
    image_grad = image_cot.astype(f32) * norm_gain
    pair_grad = swap_pair(image_grad)

    gain_row = norm_gain.reshape(1, local_cols)
    sums = row_sums(
        image_rows, pair_rows, image_grad, pair_grad, text_embed, d_normed, gain_row
    )
    sums = swap_all(sums, ("x", "y"))

    even, odd = here ^ 1, 3 - here
    shape = (X, Y, C, local_cols, local_cols)
    picks = (3 - even, even, odd ^ 1, odd, odd, here, even, here)
    image_normed, sent_a, sent_b, kept_a, kept_b = product(
        proj_weight.reshape(shape),
        pair_weight.reshape(shape),
        sums,
        (image_rows, pair_rows),
        (image_grad, pair_grad),
        gain_row,
        picks,
        core,
        model_width,
    )
    got_a = swap_even(sent_a)
    got_b = swap_odd(sent_b)

    def both(kept, got, index):
        return kept[index].astype(f32) + got[index].astype(f32)

    last_a = swap_odd(both(kept_a, got_a, 0).astype(bf16))
    last_b = swap_even(both(kept_b, got_b, 0).astype(bf16))
    over_x = combined(kept_a, got_a, last_a, kept_b, got_b, last_b)
    over_y = swap_all(over_x, "y")
    d_act = jnp.sum(over_y.astype(f32), axis=0).T
    own_hidden = lax.dynamic_slice_in_dim(hidden, lane_index * local_cols, local_cols, 1)
    d_hidden = (d_act * gelu_slope(own_hidden.astype(f32))).astype(bf16)

    outgoing = gathered(sender, image_normed)
    incoming = exchange(outgoing)
    placed = scattered(receiver, incoming).astype(bf16)

    text_sums = jnp.sum(sums[:, 2:], axis=0)
    text_sums = text_sums + swap_pair(text_sums)
    text_sq, text_cr = text_sums.reshape(2, tok_dev)
    inverse = lax.rsqrt(text_sq / model_width + epsilon)[:, None]
    cross_mean = (text_cr / model_width)[:, None]
    is_image = (doc_slot >= 0)[:, None]
    text_wide = text_embed.astype(f32)
    text_grad = d_normed.astype(f32) * norm_gain
    text_normed = (text_wide * inverse * norm_gain).astype(bf16)
    normed = jnp.where(is_image, placed, text_normed)
    d_text = inverse * (text_grad - text_wide * inverse * inverse * cross_mean)
    d_text = jnp.where(is_image, 0.0, d_text).astype(bf16)
    return (normed, d_text, d_hidden)


def solution(mesh):
    groups = mesh.shape["grp"]
    fine = Mesh(mesh.devices.reshape(groups, X, Y, C), ("grp", "x", "y", "core"))
    tp = ("x", "y", "core")
    in_specs = (
        P("grp", None),
        P(None, tp),
        P(tp),
        P(),
        P("grp", tp),
        P(tp),
        P("grp", tp),
    )
    out_specs = (P("grp", tp), P("grp", tp), P("grp", tp))

    return jax.shard_map(on_device, mesh=fine, in_specs=in_specs, out_specs=out_specs, check_vma=False)
```

```python
import jax
import jax.numpy as jnp
from jax import lax
from jax.experimental import pallas as pl
from jax.experimental.pallas import tpu as pltpu
from jax.sharding import Mesh, PartitionSpec as P


TILE = 8
X, Y, C = 4, 4, 2
LANES = 128
GRANT = 16 << 20
LARGE_GRANT = 49 << 20

epsilon = 1e-05
bf16, f32 = jnp.bfloat16, jnp.float32


def gelu(values):
    return values * (0.5 * (1.0 + lax.erf(values * 0.7071067811865476)))


def gelu_slope(values):
    normal_cdf = 0.5 * (1.0 + lax.erf(values * 0.7071067811865476))
    density = jnp.exp(-0.5 * values * values) * 0.3989422804014327
    return normal_cdf + values * density


def match_table(wanted, choices_count):
    return wanted[None, :] == jnp.arange(choices_count, dtype=jnp.int32)[:, None]


def row_sums(image_rows, image_grad, text_embed, d_normed, norm_gain):
    rows, cols = image_rows.shape
    texts = text_embed.shape[0] // rows
    count = 2 + 2 * texts

    def kernel(image_r, image_g, text_r, d_r, gain_r, o_ref):
        lane = lax.broadcasted_iota(jnp.int32, (rows, LANES), 1)
        table = jnp.zeros((rows, LANES), f32)

        def put(table, index, values):
            return jnp.where(lane == index, jnp.sum(values, axis=1, keepdims=True), table)

        wide = image_r[...].astype(f32)
        table = put(table, 0, wide * wide)
        table = put(table, 1, image_g[...] * wide)
        for i in range(texts):
            text = text_r[pl.ds(i * rows, rows), :].astype(f32)
            grad = d_r[pl.ds(i * rows, rows), :].astype(f32) * gain_r[...]
            table = put(table, 2 + i, text * text)
            table = put(table, 2 + texts + i, grad * text)
        flat = table.T[:count]
        o_ref[...] = jnp.broadcast_to(flat[None], (X * Y, count, rows))

    return pl.pallas_call(
        kernel,
        out_shape=jax.ShapeDtypeStruct((X * Y, count, rows), f32),
        compiler_params=pltpu.CompilerParams(vmem_limit_bytes=GRANT),
        cost_estimate=pl.CostEstimate(
            flops=8 * rows * cols * (texts + 2),
            bytes_accessed=4 * rows * cols * (texts + 2),
            transcendentals=0,
        ),
    )(image_rows, image_grad, text_embed, d_normed, norm_gain)


def product(own_weight, pair_weight, sums_pair, rows_pair, grads_pair, norm_gain, picks, core, width):
    features, cols = own_weight.shape[-2:]
    rows = rows_pair[0].shape[0]
    half = Y // 2
    groups, each = 4, 2

    def kernel(pick, own_0, own_1, pair_0, pair_1, own_s, pair_s, own_r, pair_r, own_g, pair_g, gain, *rest):
        normed, outs, own_d, pair_d = rest[0], rest[1:5], rest[5], rest[6]
        step = pl.program_id(0)

        @pl.when(step == 0)
        def _():
            total = own_s[...] + pair_s[...]
            full = jnp.concatenate([total, jnp.zeros((LANES - total.shape[0], rows), f32)], axis=0)
            columns = full.T
            inverse = lax.rsqrt(columns[:, 0:1] / width + epsilon)
            cross_mean = columns[:, 1:2] / width

            def gradient(wide, grad):
                d_rows = inverse * (grad - wide * inverse * inverse * cross_mean)
                return d_rows.T.astype(bf16)

            wide = own_r[...].astype(f32)
            own_d[...] = gradient(wide, own_g[...])
            pair_d[...] = gradient(pair_r[...].astype(f32), pair_g[...])
            normed[...] = (wide * inverse * gain[...]).astype(bf16)

        def part(w, d):
            return jnp.dot(w[...].reshape(half * features, cols), d[...], preferred_element_type=f32)

        totals = [
            (part(own, own_d) + part(pair, pair_d)).astype(bf16).reshape(half, features, rows)
            for own, pair in ((own_0, pair_0), (own_1, pair_1))
        ]
        for k, out in enumerate(outs):

            @pl.when(step == k)
            def _(out=out):
                for j, total in enumerate(totals):
                    out[j] = total

    def whole(*shape):
        return pl.BlockSpec(shape, lambda i, s: (0,) * len(shape))

    def weight_spec(j):
        return pl.BlockSpec(
            (None, half, None, features, cols),
            lambda i, s: (s[each * i + j], i % 2, s[groups * each], 0, 0),
        )

    return pl.pallas_call(
        kernel,
        grid_spec=pltpu.PrefetchScalarGridSpec(
            num_scalar_prefetch=1,
            grid=(groups,),
            in_specs=[weight_spec(0), weight_spec(1)] * 2
            + [whole(*sums_pair[0].shape)] * 2
            + [whole(rows, cols)] * 4
            + [whole(1, cols)],
            out_specs=[whole(rows, cols)] + [whole(each, half, features, rows)] * groups,
            scratch_shapes=[pltpu.VMEM((cols, rows), bf16)] * 2,
        ),
        out_shape=[jax.ShapeDtypeStruct((rows, cols), bf16)]
        + [jax.ShapeDtypeStruct((each, half, features, rows), bf16)] * groups,
        compiler_params=pltpu.CompilerParams(vmem_limit_bytes=LARGE_GRANT),
        cost_estimate=pl.CostEstimate(
            flops=4 * groups * each * half * features * cols * rows,
            bytes_accessed=2 * groups * each * half * features * (2 * cols + rows),
            transcendentals=rows,
        ),
    )(
        jnp.stack([*picks, core]),
        *(own_weight, own_weight, pair_weight, pair_weight),
        *sums_pair,
        *rows_pair,
        *grads_pair,
        norm_gain,
    )


def finished(over_y, slope):
    rows, cols = slope.shape

    def kernel(parts, slope_r, o_ref):
        total = jnp.sum(parts[...].astype(f32), axis=0)
        o_ref[...] = (total.T * slope_r[...]).astype(bf16)

    return pl.pallas_call(
        kernel,
        out_shape=jax.ShapeDtypeStruct((rows, cols), bf16),
        compiler_params=pltpu.CompilerParams(vmem_limit_bytes=GRANT),
        cost_estimate=pl.CostEstimate(
            flops=6 * rows * cols, bytes_accessed=14 * rows * cols, transcendentals=0
        ),
    )(over_y, slope)


def combined(kept_a, got_a, last_a, kept_b, got_b, last_b):
    half, features, rows = last_a.shape

    def kernel(kept_a, got_a, last_a, kept_b, got_b, last_b, o_ref):
        for at, parts in ((0, (kept_a, got_a, last_a)), (half, (kept_b, got_b, last_b))):
            total = sum(part[...].astype(f32) for part in parts)
            o_ref[pl.ds(at, half)] = total.astype(bf16)

    second = pl.BlockSpec((None, half, features, rows), lambda i: (1, 0, 0, 0))
    whole = pl.BlockSpec((half, features, rows), lambda i: (0, 0, 0))
    return pl.pallas_call(
        kernel,
        grid=(1,),
        in_specs=[second, second, whole] * 2,
        out_specs=pl.BlockSpec((2 * half, features, rows), lambda i: (0, 0, 0)),
        out_shape=jax.ShapeDtypeStruct((2 * half, features, rows), bf16),
        compiler_params=pltpu.CompilerParams(vmem_limit_bytes=GRANT),
        cost_estimate=pl.CostEstimate(
            flops=4 * half * features * rows,
            bytes_accessed=16 * half * features * rows,
            transcendentals=0,
        ),
    )(kept_a, got_a, last_a, kept_b, got_b, last_b)


def swap_pair(value):
    return lax.ppermute(value, "core", [(0, 1), (1, 0)])


def swap_even(value):
    return lax.ppermute(value, "x", [(i, i ^ 1) for i in range(X)])


def swap_odd(value):
    return lax.ppermute(value, "x", [(i, 3 - i) for i in range(X)])


def swap_all(value, axis):
    return lax.all_to_all(value, axis, split_axis=0, concat_axis=0, tiled=True)


def on_device(hidden, proj_weight, proj_bias, tile_pos, text_embed, norm_gain, d_normed):
    rows_dev, model_width = hidden.shape
    local_cols = proj_weight.shape[1]
    tok_dev = text_embed.shape[0]
    groups = lax.axis_size("grp")
    group_index = lax.axis_index("grp")
    core = lax.axis_index("core")
    here = lax.axis_index("x")
    lane_index = (here * Y + lax.axis_index("y")) * C + core
    tiles_dev = rows_dev // TILE
    spread = tok_dev // TILE
    total_tiles = tiles_dev * groups
    capacity = max(2, (tiles_dev + groups - 1) // groups)
    slot_rows = groups * capacity * TILE

    target = tile_pos // spread
    local_pos = tile_pos - group_index * spread
    tile_index = jnp.arange(total_tiles, dtype=jnp.int32)
    source = tile_index // tiles_dev
    earlier = (
        (source[:, None] == source[None, :])
        & (target[:, None] == target[None, :])
        & (tile_index[:, None] < tile_index[None, :])
    )
    standing = jnp.sum(earlier.astype(jnp.int32), axis=0)

    def slots_of(names, rows, slot):
        row = jnp.arange(rows, dtype=jnp.int32)
        chosen = names[:, None] == (row // TILE)[None, :]
        found = slot[:, None] * TILE + (row % TILE)[None, :] + 1
        return jnp.sum(jnp.where(chosen, found, 0), axis=0) - 1

    doc_slot = slots_of(local_pos, tok_dev, source * capacity + standing)
    image_slot = slots_of(
        tile_index - group_index * tiles_dev, rows_dev, target * capacity + standing
    )
    receiver = match_table(doc_slot, slot_rows).astype(bf16)
    sender = match_table(image_slot, slot_rows).astype(bf16)

    def gathered(table, rows):
        return jnp.dot(table, rows, preferred_element_type=f32).astype(bf16)

    def scattered(table, rows):
        return lax.dot_general(table, rows, (((0,), (0,)), ((), ())), preferred_element_type=f32)

    def exchange(rows):
        split = rows.reshape(groups, capacity * TILE, local_cols)
        return swap_all(split, "grp").reshape(slot_rows, local_cols)

    fetch_out = gathered(receiver, d_normed)
    fetch_in = exchange(fetch_out)

    pair_weight = swap_pair(proj_weight)

    activated = gelu(hidden.astype(f32)).astype(bf16)
    image_rows = jnp.dot(activated, proj_weight, preferred_element_type=f32) + proj_bias
    image_rows = image_rows.astype(bf16)

    image_cot = scattered(sender, fetch_in).astype(bf16)
    image_grad = image_cot.astype(f32) * norm_gain

    gain_row = norm_gain.reshape(1, local_cols)
    copies = row_sums(image_rows, image_grad, text_embed, d_normed, gain_row)
    sums = jnp.sum(swap_all(copies, ("x", "y")), axis=0)
    pair_sums = swap_pair(sums)
    pair_rows = swap_pair(image_rows)
    pair_grad = swap_pair(image_grad)

    even, odd = here ^ 1, 3 - here
    shape = (X, Y, C, local_cols, local_cols)
    picks = (3 - even, even, odd ^ 1, odd, odd, here, even, here)
    image_normed, sent_a, sent_b, kept_a, kept_b = product(
        proj_weight.reshape(shape),
        pair_weight.reshape(shape),
        (sums, pair_sums),
        (image_rows, pair_rows),
        (image_grad, pair_grad),
        gain_row,
        picks,
        core,
        model_width,
    )
    got_a = swap_even(sent_a)
    got_b = swap_odd(sent_b)

    def both(kept, got, index):
        return kept[index].astype(f32) + got[index].astype(f32)

    last_a = swap_odd(both(kept_a, got_a, 0).astype(bf16))
    last_b = swap_even(both(kept_b, got_b, 0).astype(bf16))
    over_x = combined(kept_a, got_a, last_a, kept_b, got_b, last_b)
    over_y = swap_all(over_x, "y")
    own_hidden = lax.dynamic_slice_in_dim(hidden, lane_index * local_cols, local_cols, 1)
    slope = gelu_slope(own_hidden.astype(f32))
    d_hidden = finished(over_y, slope)

    outgoing = gathered(sender, image_normed)
    incoming = exchange(outgoing)
    placed = scattered(receiver, incoming).astype(bf16)

    text_sums = (sums + pair_sums)[2:]
    text_sq, text_cr = text_sums.reshape(2, tok_dev)
    inverse = lax.rsqrt(text_sq / model_width + epsilon)[:, None]
    cross_mean = (text_cr / model_width)[:, None]
    is_image = (doc_slot >= 0)[:, None]
    text_wide = text_embed.astype(f32)
    text_grad = d_normed.astype(f32) * norm_gain
    text_normed = (text_wide * inverse * norm_gain).astype(bf16)
    normed = jnp.where(is_image, placed, text_normed)
    d_text = inverse * (text_grad - text_wide * inverse * inverse * cross_mean)
    d_text = jnp.where(is_image, 0.0, d_text).astype(bf16)
    return (normed, d_text, d_hidden)


def solution(mesh):
    groups = mesh.shape["grp"]
    fine = Mesh(mesh.devices.reshape(groups, X, Y, C), ("grp", "x", "y", "core"))
    tp = ("x", "y", "core")
    in_specs = (
        P("grp", None),
        P(None, tp),
        P(tp),
        P(),
        P("grp", tp),
        P(tp),
        P("grp", tp),
    )
    out_specs = (P("grp", tp), P("grp", tp), P("grp", tp))

    return jax.shard_map(on_device, mesh=fine, in_specs=in_specs, out_specs=out_specs, check_vma=False)
```

```python
import jax
import jax.numpy as jnp
from jax import lax
from jax.experimental import pallas as pl
from jax.experimental.pallas import tpu as pltpu
from jax.sharding import Mesh, PartitionSpec as P


TILE = 8
X, Y, C = 4, 4, 2
LANES = 128
GRANT = 16 << 20

epsilon = 1e-05
bf16, f32 = jnp.bfloat16, jnp.float32


def gelu(values):
    return values * (0.5 * (1.0 + lax.erf(values * 0.7071067811865476)))


def gelu_slope(values):
    normal_cdf = 0.5 * (1.0 + lax.erf(values * 0.7071067811865476))
    density = jnp.exp(-0.5 * values * values) * 0.3989422804014327
    return normal_cdf + values * density


def stays(value):
    return pltpu.with_memory_space_constraint(value, pltpu.HBM)


def match_table(wanted, choices_count):
    return wanted[None, :] == jnp.arange(choices_count, dtype=jnp.int32)[:, None]


def outset(tile_pos, group_index, d_normed, groups, capacity):
    tok_dev, cols = d_normed.shape
    total = tile_pos.shape[0]
    spread = tok_dev // TILE
    tiles_dev = total // groups
    slots = groups * capacity

    def kernel(group, pos_r, d_r, given, standing_r, document_r):
        def iota(shape, axis):
            return lax.broadcasted_iota(jnp.int32, shape, axis)

        def one_hot(truth):
            return jnp.where(truth, 1.0, 0.0).astype(bf16)

        def whole_part(values, divisor):
            return jnp.floor((values.astype(f32) + 0.5) * (1.0 / divisor))

        pos = pos_r[...]
        tile = iota((1, total), 1)
        target, source = whole_part(pos, spread), whole_part(tile, tiles_dev)
        pair = target + source * groups
        pair_column = jnp.broadcast_to(pair, (LANES, total)).T[:, :1]
        earlier = (pair_column == pair) & (iota((total, total), 0) < iota((total, total), 1))
        standing = jnp.sum(jnp.where(earlier, 1.0, 0.0), axis=0, keepdims=True).astype(jnp.int32)
        standing_r[...] = standing
        slot = source.astype(jnp.int32) * capacity + standing
        local = pos - group[0] * spread
        arrival = one_hot(iota((LANES, total), 0) == slot)
        place = one_hot(iota((LANES, total), 0) == local)
        tiles = lax.dot_general(
            arrival, place, (((1,), (1,)), ((), ())), preferred_element_type=f32
        ).astype(bf16)
        wide = (slots * TILE, LANES)
        long = (LANES, tok_dev)
        rise = one_hot((iota(wide, 0) // TILE) == iota(wide, 1))
        run = one_hot((iota(long, 1) // TILE) == iota(long, 0))
        spread_tiles = jnp.dot(rise, tiles, preferred_element_type=f32).astype(bf16)
        rows = jnp.dot(spread_tiles, run, preferred_element_type=f32)
        both = rows.shape
        same = (iota(both, 0) % TILE) == (iota(both, 1) % TILE)
        rows = jnp.where(same, rows, 0.0)
        order = (iota(both, 0) + 1).astype(f32)
        document_r[...] = jnp.sum(rows * order, axis=0, keepdims=True).astype(jnp.int32) - 1
        picked = rows.astype(bf16)
        given[...] = jnp.dot(picked, d_r[...], preferred_element_type=f32).astype(bf16)

    vmem = pl.BlockSpec(memory_space=pltpu.VMEM)
    return pl.pallas_call(
        kernel,
        in_specs=[pl.BlockSpec(memory_space=pltpu.SMEM), vmem, vmem],
        out_specs=[vmem] * 3,
        out_shape=[
            jax.ShapeDtypeStruct((slots * TILE, cols), bf16),
            jax.ShapeDtypeStruct((1, total), jnp.int32),
            jax.ShapeDtypeStruct((1, tok_dev), jnp.int32),
        ],
        compiler_params=pltpu.CompilerParams(vmem_limit_bytes=GRANT),
        cost_estimate=pl.CostEstimate(
            flops=2 * slots * TILE * tok_dev * (cols + LANES),
            bytes_accessed=2 * tok_dev * (cols + slots * TILE),
            transcendentals=0,
        ),
    )(group_index.reshape(1), tile_pos.reshape(1, total), d_normed)


def row_sums(image_rows, image_grad, text_embed, d_normed, norm_gain):
    rows, cols = image_rows.shape
    texts = text_embed.shape[0] // rows
    count = 2 + 2 * texts

    def kernel(image_r, image_g, text_r, d_r, gain_r, o_ref, packed):
        lane = lax.broadcasted_iota(jnp.int32, (rows, LANES), 1)
        table = jnp.zeros((rows, LANES), f32)

        def put(table, index, values):
            return jnp.where(lane == index, jnp.sum(values, axis=1, keepdims=True), table)

        wide = image_r[...].astype(f32)
        packed[0] = image_g[...]
        packed[1] = wide
        table = put(table, 0, wide * wide)
        table = put(table, 1, image_g[...] * wide)
        for i in range(texts):
            text = text_r[pl.ds(i * rows, rows), :].astype(f32)
            grad = d_r[pl.ds(i * rows, rows), :].astype(f32) * gain_r[...]
            table = put(table, 2 + i, text * text)
            table = put(table, 2 + texts + i, grad * text)
        flat = table.T[:count]
        o_ref[...] = jnp.broadcast_to(flat[None], (X * Y * C, count, rows))

    return pl.pallas_call(
        kernel,
        out_shape=[
            jax.ShapeDtypeStruct((X * Y * C, count, rows), f32),
            jax.ShapeDtypeStruct((2, rows, cols), f32),
        ],
        compiler_params=pltpu.CompilerParams(vmem_limit_bytes=GRANT),
        cost_estimate=pl.CostEstimate(
            flops=8 * rows * cols * (texts + 2),
            bytes_accessed=4 * rows * cols * (texts + 2),
            transcendentals=0,
        ),
    )(image_rows, image_grad, text_embed, d_normed, norm_gain)


def products(own_weight, pair_weight, inputs, picks, core, slot_rows=None, width=None):
    features, cols = own_weight.shape[-2:]
    half, groups, each = Y // 2, 2, 2
    rows = inputs[0].shape[1] if slot_rows else inputs[1].shape[0]

    def fetches(pick, weights, blocks, sems):
        copies = []
        for n in range(groups * each):
            from_y = pl.ds(n // each * half, half)
            copies.append(
                [
                    pltpu.make_async_copy(
                        weight.at[pick[n], from_y, pick[groups * each]],
                        blocks.at[m, n],
                        sems.at[m, n],
                    )
                    for m, weight in enumerate(weights)
                ]
            )
        for pair in copies:
            for copy in pair:
                copy.start()
        return copies

    def put(copies, blocks, gradients, outs):
        for n, pair in enumerate(copies):
            total = 0.0
            for m, copy in enumerate(pair):
                copy.wait()
                w = blocks[m, n].reshape(half * features, cols)
                total = total + jnp.dot(w, gradients[m][...], preferred_element_type=f32)
            outs[n // each][n % each] = total.astype(bf16).reshape(half, features, rows)

    def first(pick, own_w, pair_w, sums, own_r, own_g, packed, gain, out_a, out_b, own_d, pair_d, normed, blocks, sems):
        copies = fetches(pick, (own_w, pair_w), blocks, sems)
        total = jnp.sum(sums[...], axis=0)
        full = jnp.concatenate([total, jnp.zeros((LANES - total.shape[0], rows), f32)], axis=0)
        columns = full.T
        inverse = lax.rsqrt(columns[:, 0:1] / width + epsilon)
        cross_mean = columns[:, 1:2] / width

        def gradient(wide, grad):
            d_rows = inverse * (grad - wide * inverse * inverse * cross_mean)
            return d_rows.T.astype(bf16)

        wide = own_r[...].astype(f32)
        own_d[...] = gradient(wide, own_g[...])
        pair_d[...] = gradient(packed[1], packed[0])
        put(copies, blocks, (own_d, pair_d), (out_a, out_b))
        normed[...] = (wide * inverse * gain[...]).astype(bf16)

    def second(pick, own_w, pair_w, own_d, pair_d, normed, slot, out_a, out_b, outgoing, blocks, sems):
        copies = fetches(pick, (own_w, pair_w), blocks, sems)
        sender = lax.broadcasted_iota(jnp.int32, (outgoing.shape[0], rows), 0) == slot[...]
        sender = jnp.where(sender, 1.0, 0.0).astype(bf16)
        outgoing[...] = jnp.dot(sender, normed[...], preferred_element_type=f32).astype(bf16)
        put(copies, blocks, (own_d, pair_d), (out_a, out_b))

    out_shape = [jax.ShapeDtypeStruct((each, half, features, rows), bf16)] * groups
    if slot_rows:
        out_shape += [jax.ShapeDtypeStruct((slot_rows, cols), bf16)]
    else:
        out_shape += [pltpu.HBM((cols, rows), bf16)] * 2
        out_shape += [pltpu.HBM((rows, cols), bf16)]
    vmem, hbm = pl.BlockSpec(memory_space=pltpu.VMEM), pl.BlockSpec(memory_space=pltpu.HBM)
    return pl.pallas_call(
        second if slot_rows else first,
        in_specs=[pl.BlockSpec(memory_space=pltpu.SMEM), hbm, hbm] + [vmem] * len(inputs),
        out_specs=[vmem] * len(out_shape),
        out_shape=out_shape,
        scratch_shapes=[
            pltpu.VMEM((C, groups * each, half, features, cols), bf16),
            pltpu.SemaphoreType.DMA((C, groups * each)),
        ],
        compiler_params=pltpu.CompilerParams(vmem_limit_bytes=GRANT),
        cost_estimate=pl.CostEstimate(
            flops=4 * groups * each * half * features * cols * rows,
            bytes_accessed=2 * groups * each * half * features * (2 * cols + rows),
            transcendentals=rows,
        ),
    )(
        jnp.stack([*picks, core]),
        *(stays(weight) for weight in (own_weight, pair_weight)),
        *(stays(value) if slot_rows else value for value in inputs),
    )


def finished(over_y, slope):
    rows, cols = slope.shape

    def kernel(parts, slope_r, o_ref):
        total = jnp.sum(parts[...].astype(f32), axis=0)
        o_ref[...] = (total.T * slope_r[...]).astype(bf16)

    return pl.pallas_call(
        kernel,
        out_shape=jax.ShapeDtypeStruct((rows, cols), bf16),
        compiler_params=pltpu.CompilerParams(vmem_limit_bytes=GRANT),
        cost_estimate=pl.CostEstimate(
            flops=6 * rows * cols, bytes_accessed=14 * rows * cols, transcendentals=0
        ),
    )(over_y, slope)


def combined(kept_a, got_a, last_a, kept_b, got_b, last_b):
    half, features, rows = last_a.shape

    def kernel(kept_a, got_a, last_a, kept_b, got_b, last_b, o_ref):
        for at, parts in ((0, (kept_a, got_a, last_a)), (half, (kept_b, got_b, last_b))):
            total = sum(part[...].astype(f32) for part in parts)
            o_ref[pl.ds(at, half)] = total.astype(bf16)

    second = pl.BlockSpec((None, half, features, rows), lambda i: (1, 0, 0, 0))
    whole = pl.BlockSpec((half, features, rows), lambda i: (0, 0, 0))
    return pl.pallas_call(
        kernel,
        grid=(1,),
        in_specs=[second, second, whole] * 2,
        out_specs=pl.BlockSpec((2 * half, features, rows), lambda i: (0, 0, 0)),
        out_shape=jax.ShapeDtypeStruct((2 * half, features, rows), bf16),
        compiler_params=pltpu.CompilerParams(vmem_limit_bytes=GRANT),
        cost_estimate=pl.CostEstimate(
            flops=4 * half * features * rows,
            bytes_accessed=16 * half * features * rows,
            transcendentals=0,
        ),
    )(kept_a, got_a, last_a, kept_b, got_b, last_b)


def swap_pair(value):
    return lax.ppermute(value, "core", [(0, 1), (1, 0)])


def swap_even(value):
    return lax.ppermute(value, "x", [(i, i ^ 1) for i in range(X)])


def swap_odd(value):
    return lax.ppermute(value, "x", [(i, 3 - i) for i in range(X)])


def swap_all(value, axis):
    return lax.all_to_all(value, axis, split_axis=0, concat_axis=0, tiled=True)


def on_device(hidden, proj_weight, proj_bias, tile_pos, text_embed, norm_gain, d_normed):
    rows_dev, model_width = hidden.shape
    local_cols = proj_weight.shape[1]
    tok_dev = text_embed.shape[0]
    groups = lax.axis_size("grp")
    group_index = lax.axis_index("grp")
    core = lax.axis_index("core")
    here = lax.axis_index("x")
    lane_index = (here * Y + lax.axis_index("y")) * C + core
    tiles_dev = rows_dev // TILE
    spread = tok_dev // TILE
    total_tiles = tiles_dev * groups
    capacity = max(2, (tiles_dev + groups - 1) // groups)
    slot_rows = groups * capacity * TILE

    fetch_out, standing, doc_slot = outset(tile_pos, group_index, d_normed, groups, capacity)
    tile_index = jnp.arange(total_tiles, dtype=jnp.int32)
    slot = tile_pos // spread * capacity + standing[0]
    receiver = (doc_slot == jnp.arange(slot_rows, dtype=jnp.int32)[:, None]).astype(bf16)
    row = jnp.arange(rows_dev, dtype=jnp.int32)
    own_tile = (tile_index - group_index * tiles_dev)[:, None] == (row // TILE)[None, :]
    found = slot[:, None] * TILE + (row % TILE)[None, :]
    image_slot = jnp.sum(jnp.where(own_tile, found, 0), axis=0)
    sender = match_table(image_slot, slot_rows).astype(bf16)

    def scattered(table, rows):
        return lax.dot_general(table, rows, (((0,), (0,)), ((), ())), preferred_element_type=f32)

    def exchange(rows):
        split = rows.reshape(groups, capacity * TILE, local_cols)
        return swap_all(split, "grp").reshape(slot_rows, local_cols)

    fetch_in = exchange(fetch_out)

    pair_weight = swap_pair(proj_weight)

    activated = gelu(hidden.astype(f32)).astype(bf16)
    image_rows = jnp.dot(activated, proj_weight, preferred_element_type=f32) + proj_bias
    image_rows = image_rows.astype(bf16)

    image_cot = scattered(sender, fetch_in).astype(bf16)
    image_grad = image_cot.astype(f32) * norm_gain

    gain_row = norm_gain.reshape(1, local_cols)
    copies, packed = row_sums(image_rows, image_grad, text_embed, d_normed, gain_row)
    sums = swap_all(copies, ("x", "y", "core"))
    pair_image = swap_pair(packed)

    even, odd = here ^ 1, 3 - here
    shape = (X, Y, C, local_cols, local_cols)
    own_weight, pair_weight = proj_weight.reshape(shape), pair_weight.reshape(shape)
    sent_a, sent_b, own_d, pair_d, image_normed = products(
        own_weight,
        pair_weight,
        (sums, image_rows, image_grad, pair_image, gain_row),
        (3 - even, even, odd ^ 1, odd),
        core,
        width=model_width,
    )
    got_a = swap_even(sent_a)
    got_b = swap_odd(sent_b)

    kept_a, kept_b, outgoing = products(
        own_weight,
        pair_weight,
        (own_d, pair_d, image_normed, image_slot.reshape(1, rows_dev)),
        (odd, here, even, here),
        core,
        slot_rows=slot_rows,
    )

    def both(kept, got, index):
        return kept[index].astype(f32) + got[index].astype(f32)

    last_a = swap_odd(both(kept_a, got_a, 0).astype(bf16))
    last_b = swap_even(both(kept_b, got_b, 0).astype(bf16))
    over_x = combined(kept_a, got_a, last_a, kept_b, got_b, last_b)
    over_y = swap_all(over_x, "y")
    own_hidden = lax.dynamic_slice_in_dim(hidden, lane_index * local_cols, local_cols, 1)
    slope = gelu_slope(own_hidden.astype(f32))
    d_hidden = finished(over_y, slope)

    incoming = exchange(outgoing)
    placed = scattered(receiver, incoming).astype(bf16)

    text_sums = jnp.sum(sums[:, 2:], axis=0)
    text_sq, text_cr = text_sums.reshape(2, tok_dev)
    inverse = lax.rsqrt(text_sq / model_width + epsilon)[:, None]
    cross_mean = (text_cr / model_width)[:, None]
    is_image = (doc_slot >= 0).reshape(tok_dev, 1)
    text_wide = text_embed.astype(f32)
    text_grad = d_normed.astype(f32) * norm_gain
    text_normed = (text_wide * inverse * norm_gain).astype(bf16)
    normed = jnp.where(is_image, placed, text_normed)
    d_text = inverse * (text_grad - text_wide * inverse * inverse * cross_mean)
    d_text = jnp.where(is_image, 0.0, d_text).astype(bf16)
    return (normed, d_text, d_hidden)


def solution(mesh):
    groups = mesh.shape["grp"]
    fine = Mesh(mesh.devices.reshape(groups, X, Y, C), ("grp", "x", "y", "core"))
    tp = ("x", "y", "core")
    in_specs = (
        P("grp", None),
        P(None, tp),
        P(tp),
        P(),
        P("grp", tp),
        P(tp),
        P("grp", tp),
    )
    out_specs = (P("grp", tp), P("grp", tp), P("grp", tp))

    return jax.shard_map(on_device, mesh=fine, in_specs=in_specs, out_specs=out_specs, check_vma=False)
```

```python
import jax
import jax.numpy as jnp
from jax import lax
from jax.experimental import pallas as pl
from jax.experimental.pallas import tpu as pltpu
from jax.sharding import Mesh, PartitionSpec as P


TILE = 8
X, Y, C = 4, 4, 2
LANES = 128
GRANT = 16 << 20

epsilon = 1e-05
bf16, f32 = jnp.bfloat16, jnp.float32


def gelu(values):
    return values * (0.5 * (1.0 + lax.erf(values * 0.7071067811865476)))


def gelu_slope(values):
    normal_cdf = 0.5 * (1.0 + lax.erf(values * 0.7071067811865476))
    density = jnp.exp(-0.5 * values * values) * 0.3989422804014327
    return normal_cdf + values * density


def stays(value):
    return pltpu.with_memory_space_constraint(value, pltpu.HBM)


def match_table(wanted, choices_count):
    return wanted[None, :] == jnp.arange(choices_count, dtype=jnp.int32)[:, None]


def outset(tile_pos, group_index, d_normed, groups, capacity):
    tok_dev, cols = d_normed.shape
    total = tile_pos.shape[0]
    spread = tok_dev // TILE
    tiles_dev = total // groups
    slots = groups * capacity

    def kernel(group, pos_r, d_r, given, standing_r, document_r, d_rows, sem):
        copy = pltpu.make_async_copy(d_r, d_rows, sem)
        copy.start()

        def iota(shape, axis):
            return lax.broadcasted_iota(jnp.int32, shape, axis)

        def one_hot(truth):
            return jnp.where(truth, 1.0, 0.0).astype(bf16)

        def whole_part(values, divisor):
            return jnp.floor((values.astype(f32) + 0.5) * (1.0 / divisor))

        pos = pos_r[...]
        tile = iota((1, total), 1)
        target, source = whole_part(pos, spread), whole_part(tile, tiles_dev)
        pair = target + source * groups
        pair_column = jnp.broadcast_to(pair, (LANES, total)).T[:, :1]
        earlier = (pair_column == pair) & (iota((total, total), 0) < iota((total, total), 1))
        standing = jnp.sum(jnp.where(earlier, 1.0, 0.0), axis=0, keepdims=True).astype(jnp.int32)
        standing_r[...] = standing
        slot = source.astype(jnp.int32) * capacity + standing
        local = pos - group[0] * spread
        arrival = one_hot(iota((LANES, total), 0) == slot)
        place = one_hot(iota((LANES, total), 0) == local)
        tiles = lax.dot_general(
            arrival, place, (((1,), (1,)), ((), ())), preferred_element_type=f32
        ).astype(bf16)
        wide = (slots * TILE, LANES)
        long = (LANES, tok_dev)
        rise = one_hot((iota(wide, 0) // TILE) == iota(wide, 1))
        run = one_hot((iota(long, 1) // TILE) == iota(long, 0))
        spread_tiles = jnp.dot(rise, tiles, preferred_element_type=f32).astype(bf16)
        rows = jnp.dot(spread_tiles, run, preferred_element_type=f32)
        both = rows.shape
        same = (iota(both, 0) % TILE) == (iota(both, 1) % TILE)
        rows = jnp.where(same, rows, 0.0)
        order = (iota(both, 0) + 1).astype(f32)
        document_r[...] = jnp.sum(rows * order, axis=0, keepdims=True).astype(jnp.int32) - 1
        picked = rows.astype(bf16)
        copy.wait()
        given[...] = jnp.dot(picked, d_rows[...], preferred_element_type=f32).astype(bf16)

    vmem = pl.BlockSpec(memory_space=pltpu.VMEM)
    return pl.pallas_call(
        kernel,
        in_specs=[
            pl.BlockSpec(memory_space=pltpu.SMEM),
            vmem,
            pl.BlockSpec(memory_space=pltpu.HBM),
        ],
        out_specs=[vmem] * 3,
        scratch_shapes=[pltpu.VMEM((tok_dev, cols), bf16), pltpu.SemaphoreType.DMA],
        out_shape=[
            jax.ShapeDtypeStruct((slots * TILE, cols), bf16),
            jax.ShapeDtypeStruct((1, total), jnp.int32),
            jax.ShapeDtypeStruct((1, tok_dev), jnp.int32),
        ],
        compiler_params=pltpu.CompilerParams(vmem_limit_bytes=GRANT),
        cost_estimate=pl.CostEstimate(
            flops=2 * slots * TILE * tok_dev * (cols + LANES),
            bytes_accessed=2 * tok_dev * (cols + slots * TILE),
            transcendentals=0,
        ),
    )(group_index.reshape(1), tile_pos.reshape(1, total), stays(d_normed))


def row_sums(image_rows, image_grad, text_embed, d_normed, norm_gain):
    rows, cols = image_rows.shape
    texts = text_embed.shape[0] // rows
    count = 2 + 2 * texts

    def kernel(image_r, image_g, text_r, d_r, gain_r, o_ref, packed):
        lane = lax.broadcasted_iota(jnp.int32, (rows, LANES), 1)
        table = jnp.zeros((rows, LANES), f32)

        def put(table, index, values):
            return jnp.where(lane == index, jnp.sum(values, axis=1, keepdims=True), table)

        wide = image_r[...].astype(f32)
        packed[0] = image_g[...]
        packed[1] = wide
        table = put(table, 0, wide * wide)
        table = put(table, 1, image_g[...] * wide)
        for i in range(texts):
            text = text_r[pl.ds(i * rows, rows), :].astype(f32)
            grad = d_r[pl.ds(i * rows, rows), :].astype(f32) * gain_r[...]
            table = put(table, 2 + i, text * text)
            table = put(table, 2 + texts + i, grad * text)
        flat = table.T[:count]
        o_ref[...] = jnp.broadcast_to(flat[None], (X * C, count, rows))

    return pl.pallas_call(
        kernel,
        out_shape=[
            jax.ShapeDtypeStruct((X * C, count, rows), f32),
            jax.ShapeDtypeStruct((2, rows, cols), f32),
        ],
        compiler_params=pltpu.CompilerParams(vmem_limit_bytes=GRANT),
        cost_estimate=pl.CostEstimate(
            flops=8 * rows * cols * (texts + 2),
            bytes_accessed=4 * rows * cols * (texts + 2),
            transcendentals=0,
        ),
    )(image_rows, image_grad, text_embed, d_normed, norm_gain)


def summed(parts, copies):
    _, count, rows = parts.shape

    def kernel(parts_r, o_ref):
        o_ref[...] = jnp.broadcast_to(jnp.sum(parts_r[...], axis=0)[None], (copies, count, rows))

    return pl.pallas_call(
        kernel,
        out_shape=jax.ShapeDtypeStruct((copies, count, rows), f32),
        compiler_params=pltpu.CompilerParams(vmem_limit_bytes=GRANT),
        cost_estimate=pl.CostEstimate(
            flops=parts.size, bytes_accessed=4 * (parts.size + copies * count * rows), transcendentals=0
        ),
    )(parts)


def products(own_weight, pair_weight, inputs, picks, core, slot_rows=None, width=None):
    features, cols = own_weight.shape[-2:]
    half, groups, each = Y // 2, 2, 2
    rows = inputs[0].shape[1] if slot_rows else inputs[1].shape[0]

    def fetches(pick, weights, blocks, sems):
        copies = []
        for n in range(groups * each):
            from_y = pl.ds(n // each * half, half)
            copies.append(
                [
                    pltpu.make_async_copy(
                        weight.at[pick[n], from_y, pick[groups * each]],
                        blocks.at[m, n],
                        sems.at[m, n],
                    )
                    for m, weight in enumerate(weights)
                ]
            )
        for pair in copies:
            for copy in pair:
                copy.start()
        return copies

    def put(copies, blocks, gradients, outs):
        for n, pair in enumerate(copies):
            total = 0.0
            for m, copy in enumerate(pair):
                copy.wait()
                w = blocks[m, n].reshape(half * features, cols)
                total = total + jnp.dot(w, gradients[m][...], preferred_element_type=f32)
            outs[n // each][n % each] = total.astype(bf16).reshape(half, features, rows)

    def first(pick, own_w, pair_w, sums, own_r, own_g, packed, gain, out_a, out_b, own_d, pair_d, normed, blocks, sems):
        copies = fetches(pick, (own_w, pair_w), blocks, sems)
        total = jnp.sum(sums[...], axis=0)
        full = jnp.concatenate([total, jnp.zeros((LANES - total.shape[0], rows), f32)], axis=0)
        columns = full.T
        inverse = lax.rsqrt(columns[:, 0:1] / width + epsilon)
        cross_mean = columns[:, 1:2] / width

        def gradient(wide, grad):
            d_rows = inverse * (grad - wide * inverse * inverse * cross_mean)
            return d_rows.T.astype(bf16)

        wide = own_r[...].astype(f32)
        own_d[...] = gradient(wide, own_g[...])
        pair_d[...] = gradient(packed[1], packed[0])
        put(copies, blocks, (own_d, pair_d), (out_a, out_b))
        normed[...] = (wide * inverse * gain[...]).astype(bf16)

    def second(pick, own_w, pair_w, own_d, pair_d, normed, slot, out_a, out_b, outgoing, blocks, sems):
        copies = fetches(pick, (own_w, pair_w), blocks, sems)
        sender = lax.broadcasted_iota(jnp.int32, (outgoing.shape[0], rows), 0) == slot[...]
        sender = jnp.where(sender, 1.0, 0.0).astype(bf16)
        outgoing[...] = jnp.dot(sender, normed[...], preferred_element_type=f32).astype(bf16)
        put(copies, blocks, (own_d, pair_d), (out_a, out_b))

    out_shape = [jax.ShapeDtypeStruct((each, half, features, rows), bf16)] * groups
    if slot_rows:
        out_shape += [jax.ShapeDtypeStruct((slot_rows, cols), bf16)]
    else:
        out_shape += [pltpu.HBM((cols, rows), bf16)] * 2
        out_shape += [pltpu.HBM((rows, cols), bf16)]
    vmem, hbm = pl.BlockSpec(memory_space=pltpu.VMEM), pl.BlockSpec(memory_space=pltpu.HBM)
    return pl.pallas_call(
        second if slot_rows else first,
        in_specs=[pl.BlockSpec(memory_space=pltpu.SMEM), hbm, hbm] + [vmem] * len(inputs),
        out_specs=[vmem] * len(out_shape),
        out_shape=out_shape,
        scratch_shapes=[
            pltpu.VMEM((C, groups * each, half, features, cols), bf16),
            pltpu.SemaphoreType.DMA((C, groups * each)),
        ],
        compiler_params=pltpu.CompilerParams(vmem_limit_bytes=GRANT),
        cost_estimate=pl.CostEstimate(
            flops=4 * groups * each * half * features * cols * rows,
            bytes_accessed=2 * groups * each * half * features * (2 * cols + rows),
            transcendentals=rows,
        ),
    )(
        jnp.stack([*picks, core]),
        *(stays(weight) for weight in (own_weight, pair_weight)),
        *(stays(value) if slot_rows else value for value in inputs),
    )


def finished(over_y, slope):
    rows, cols = slope.shape

    def kernel(parts, slope_r, o_ref):
        total = jnp.sum(parts[...].astype(f32), axis=0)
        o_ref[...] = (total.T * slope_r[...]).astype(bf16)

    return pl.pallas_call(
        kernel,
        out_shape=jax.ShapeDtypeStruct((rows, cols), bf16),
        compiler_params=pltpu.CompilerParams(vmem_limit_bytes=GRANT),
        cost_estimate=pl.CostEstimate(
            flops=6 * rows * cols, bytes_accessed=14 * rows * cols, transcendentals=0
        ),
    )(over_y, slope)


def combined(kept_a, got_a, last_a, kept_b, got_b, last_b):
    half, features, rows = last_a.shape

    def kernel(kept_a, got_a, last_a, kept_b, got_b, last_b, o_ref):
        for at, parts in ((0, (kept_a, got_a, last_a)), (half, (kept_b, got_b, last_b))):
            total = sum(part[...].astype(f32) for part in parts)
            o_ref[pl.ds(at, half)] = total.astype(bf16)

    second = pl.BlockSpec((None, half, features, rows), lambda i: (1, 0, 0, 0))
    whole = pl.BlockSpec((half, features, rows), lambda i: (0, 0, 0))
    return pl.pallas_call(
        kernel,
        grid=(1,),
        in_specs=[second, second, whole] * 2,
        out_specs=pl.BlockSpec((2 * half, features, rows), lambda i: (0, 0, 0)),
        out_shape=jax.ShapeDtypeStruct((2 * half, features, rows), bf16),
        compiler_params=pltpu.CompilerParams(vmem_limit_bytes=GRANT),
        cost_estimate=pl.CostEstimate(
            flops=4 * half * features * rows,
            bytes_accessed=16 * half * features * rows,
            transcendentals=0,
        ),
    )(kept_a, got_a, last_a, kept_b, got_b, last_b)


def swap_pair(value):
    return lax.ppermute(value, "core", [(0, 1), (1, 0)])


def swap_even(value):
    return lax.ppermute(value, "x", [(i, i ^ 1) for i in range(X)])


def swap_odd(value):
    return lax.ppermute(value, "x", [(i, 3 - i) for i in range(X)])


def swap_all(value, axis):
    return lax.all_to_all(value, axis, split_axis=0, concat_axis=0, tiled=True)


def on_device(hidden, proj_weight, proj_bias, tile_pos, text_embed, norm_gain, d_normed):
    rows_dev, model_width = hidden.shape
    local_cols = proj_weight.shape[1]
    tok_dev = text_embed.shape[0]
    groups = lax.axis_size("grp")
    group_index = lax.axis_index("grp")
    core = lax.axis_index("core")
    here = lax.axis_index("x")
    lane_index = (here * Y + lax.axis_index("y")) * C + core
    tiles_dev = rows_dev // TILE
    spread = tok_dev // TILE
    total_tiles = tiles_dev * groups
    capacity = max(2, (tiles_dev + groups - 1) // groups)
    slot_rows = groups * capacity * TILE

    fetch_out, standing, doc_slot = outset(tile_pos, group_index, d_normed, groups, capacity)
    tile_index = jnp.arange(total_tiles, dtype=jnp.int32)
    slot = tile_pos // spread * capacity + standing[0]
    receiver = (doc_slot == jnp.arange(slot_rows, dtype=jnp.int32)[:, None]).astype(bf16)
    row = jnp.arange(rows_dev, dtype=jnp.int32)
    own_tile = (tile_index - group_index * tiles_dev)[:, None] == (row // TILE)[None, :]
    found = slot[:, None] * TILE + (row % TILE)[None, :]
    image_slot = jnp.sum(jnp.where(own_tile, found, 0), axis=0)
    sender = match_table(image_slot, slot_rows).astype(bf16)

    def scattered(table, rows):
        return lax.dot_general(table, rows, (((0,), (0,)), ((), ())), preferred_element_type=f32)

    def exchange(rows):
        split = rows.reshape(groups, capacity * TILE, local_cols)
        return swap_all(split, "grp").reshape(slot_rows, local_cols)

    fetch_in = exchange(fetch_out)

    pair_weight = swap_pair(proj_weight)

    activated = gelu(hidden.astype(f32)).astype(bf16)
    image_rows = jnp.dot(activated, proj_weight, preferred_element_type=f32) + proj_bias
    image_rows = image_rows.astype(bf16)

    image_cot = scattered(sender, fetch_in).astype(bf16)
    image_grad = image_cot.astype(f32) * norm_gain

    gain_row = norm_gain.reshape(1, local_cols)
    copies, packed = row_sums(image_rows, image_grad, text_embed, d_normed, gain_row)
    sums = swap_all(copies, ("x", "core"))
    sums = swap_all(summed(sums, Y), "y")
    pair_image = swap_pair(packed)

    even, odd = here ^ 1, 3 - here
    shape = (X, Y, C, local_cols, local_cols)
    own_weight, pair_weight = proj_weight.reshape(shape), pair_weight.reshape(shape)
    sent_a, sent_b, own_d, pair_d, image_normed = products(
        own_weight,
        pair_weight,
        (sums, image_rows, image_grad, pair_image, gain_row),
        (3 - even, even, odd ^ 1, odd),
        core,
        width=model_width,
    )
    got_a = swap_even(sent_a)
    got_b = swap_odd(sent_b)

    kept_a, kept_b, outgoing = products(
        own_weight,
        pair_weight,
        (own_d, pair_d, image_normed, image_slot.reshape(1, rows_dev)),
        (odd, here, even, here),
        core,
        slot_rows=slot_rows,
    )

    def both(kept, got, index):
        return kept[index].astype(f32) + got[index].astype(f32)

    last_a = swap_odd(both(kept_a, got_a, 0).astype(bf16))
    last_b = swap_even(both(kept_b, got_b, 0).astype(bf16))
    over_x = combined(kept_a, got_a, last_a, kept_b, got_b, last_b)
    over_y = swap_all(over_x, "y")
    own_hidden = lax.dynamic_slice_in_dim(hidden, lane_index * local_cols, local_cols, 1)
    slope = gelu_slope(own_hidden.astype(f32))
    d_hidden = finished(over_y, slope)

    incoming = exchange(outgoing)
    placed = scattered(receiver, incoming).astype(bf16)

    text_sums = jnp.sum(sums[:, 2:], axis=0)
    text_sq, text_cr = text_sums.reshape(2, tok_dev)
    inverse = lax.rsqrt(text_sq / model_width + epsilon)[:, None]
    cross_mean = (text_cr / model_width)[:, None]
    is_image = (doc_slot >= 0).reshape(tok_dev, 1)
    text_wide = text_embed.astype(f32)
    text_grad = d_normed.astype(f32) * norm_gain
    text_normed = (text_wide * inverse * norm_gain).astype(bf16)
    normed = jnp.where(is_image, placed, text_normed)
    d_text = inverse * (text_grad - text_wide * inverse * inverse * cross_mean)
    d_text = jnp.where(is_image, 0.0, d_text).astype(bf16)
    return (normed, d_text, d_hidden)


def solution(mesh):
    groups = mesh.shape["grp"]
    fine = Mesh(mesh.devices.reshape(groups, X, Y, C), ("grp", "x", "y", "core"))
    tp = ("x", "y", "core")
    in_specs = (
        P("grp", None),
        P(None, tp),
        P(tp),
        P(),
        P("grp", tp),
        P(tp),
        P("grp", tp),
    )
    out_specs = (P("grp", tp), P("grp", tp), P("grp", tp))

    return jax.shard_map(on_device, mesh=fine, in_specs=in_specs, out_specs=out_specs, check_vma=False)
```

```python
import jax
import jax.numpy as jnp
from jax import lax
from jax.experimental import pallas as pl
from jax.experimental.pallas import tpu as pltpu
from jax.sharding import Mesh, PartitionSpec as P


TILE = 8
X, Y, C = 4, 4, 2
LANES = 128
GRANT = 16 << 20

epsilon = 1e-05
bf16, f32 = jnp.bfloat16, jnp.float32


def gelu(values):
    return values * (0.5 * (1.0 + lax.erf(values * 0.7071067811865476)))


def gelu_slope(values):
    normal_cdf = 0.5 * (1.0 + lax.erf(values * 0.7071067811865476))
    density = jnp.exp(-0.5 * values * values) * 0.3989422804014327
    return normal_cdf + values * density


def stays(value):
    return pltpu.with_memory_space_constraint(value, pltpu.HBM)


def match_table(wanted, choices_count):
    return wanted[None, :] == jnp.arange(choices_count, dtype=jnp.int32)[:, None]


def outset(tile_pos, group_index, d_normed, groups, capacity):
    tok_dev, cols = d_normed.shape
    total = tile_pos.shape[0]
    spread = tok_dev // TILE
    tiles_dev = total // groups
    slots = groups * capacity

    def kernel(group, pos_r, d_r, given, standing_r, document_r, d_rows, sem):
        copy = pltpu.make_async_copy(d_r, d_rows, sem)
        copy.start()

        def iota(shape, axis):
            return lax.broadcasted_iota(jnp.int32, shape, axis)

        def one_hot(truth):
            return jnp.where(truth, 1.0, 0.0).astype(bf16)

        def whole_part(values, divisor):
            return jnp.floor((values.astype(f32) + 0.5) * (1.0 / divisor))

        pos = pos_r[...]
        tile = iota((1, total), 1)
        target, source = whole_part(pos, spread), whole_part(tile, tiles_dev)
        pair = target + source * groups
        pair_column = jnp.broadcast_to(pair, (LANES, total)).T[:, :1]
        earlier = (pair_column == pair) & (iota((total, total), 0) < iota((total, total), 1))
        standing = jnp.sum(jnp.where(earlier, 1.0, 0.0), axis=0, keepdims=True).astype(jnp.int32)
        standing_r[...] = standing
        slot = source.astype(jnp.int32) * capacity + standing
        local = pos - group[0] * spread
        arrival = one_hot(iota((LANES, total), 0) == slot)
        place = one_hot(iota((LANES, total), 0) == local)
        tiles = lax.dot_general(
            arrival, place, (((1,), (1,)), ((), ())), preferred_element_type=f32
        ).astype(bf16)
        wide = (slots * TILE, LANES)
        long = (LANES, tok_dev)
        rise = one_hot((iota(wide, 0) // TILE) == iota(wide, 1))
        run = one_hot((iota(long, 1) // TILE) == iota(long, 0))
        spread_tiles = jnp.dot(rise, tiles, preferred_element_type=f32).astype(bf16)
        rows = jnp.dot(spread_tiles, run, preferred_element_type=f32)
        both = rows.shape
        same = (iota(both, 0) % TILE) == (iota(both, 1) % TILE)
        rows = jnp.where(same, rows, 0.0)
        order = (iota(both, 0) + 1).astype(f32)
        document_r[...] = jnp.sum(rows * order, axis=0, keepdims=True).astype(jnp.int32) - 1
        picked = rows.astype(bf16)
        copy.wait()
        given[...] = jnp.dot(picked, d_rows[...], preferred_element_type=f32).astype(bf16)

    vmem = pl.BlockSpec(memory_space=pltpu.VMEM)
    return pl.pallas_call(
        kernel,
        in_specs=[
            pl.BlockSpec(memory_space=pltpu.SMEM),
            vmem,
            pl.BlockSpec(memory_space=pltpu.HBM),
        ],
        out_specs=[vmem] * 3,
        scratch_shapes=[pltpu.VMEM((tok_dev, cols), bf16), pltpu.SemaphoreType.DMA],
        out_shape=[
            jax.ShapeDtypeStruct((slots * TILE, cols), bf16),
            jax.ShapeDtypeStruct((1, total), jnp.int32),
            jax.ShapeDtypeStruct((1, tok_dev), jnp.int32),
        ],
        compiler_params=pltpu.CompilerParams(vmem_limit_bytes=GRANT),
        cost_estimate=pl.CostEstimate(
            flops=2 * slots * TILE * tok_dev * (cols + LANES),
            bytes_accessed=2 * tok_dev * (cols + slots * TILE),
            transcendentals=0,
        ),
    )(group_index.reshape(1), tile_pos.reshape(1, total), stays(d_normed))


def row_sums(image_rows, image_grad, text_embed, d_normed, norm_gain):
    rows, cols = image_rows.shape
    texts = text_embed.shape[0] // rows
    count = 2 + 2 * texts

    def kernel(image_r, image_g, text_r, d_r, gain_r, o_ref, packed):
        lane = lax.broadcasted_iota(jnp.int32, (rows, LANES), 1)
        table = jnp.zeros((rows, LANES), f32)

        def put(table, index, values):
            return jnp.where(lane == index, jnp.sum(values, axis=1, keepdims=True), table)

        wide = image_r[...].astype(f32)
        packed[0] = image_g[...]
        packed[1] = wide
        table = put(table, 0, wide * wide)
        table = put(table, 1, image_g[...] * wide)
        for i in range(texts):
            text = text_r[pl.ds(i * rows, rows), :].astype(f32)
            grad = d_r[pl.ds(i * rows, rows), :].astype(f32) * gain_r[...]
            table = put(table, 2 + i, text * text)
            table = put(table, 2 + texts + i, grad * text)
        flat = table.T[:count]
        o_ref[...] = jnp.broadcast_to(flat[None], (X * C, count, rows))

    return pl.pallas_call(
        kernel,
        out_shape=[
            jax.ShapeDtypeStruct((X * C, count, rows), f32),
            jax.ShapeDtypeStruct((2, rows, cols), f32),
        ],
        compiler_params=pltpu.CompilerParams(vmem_limit_bytes=GRANT),
        cost_estimate=pl.CostEstimate(
            flops=8 * rows * cols * (texts + 2),
            bytes_accessed=4 * rows * cols * (texts + 2),
            transcendentals=0,
        ),
    )(image_rows, image_grad, text_embed, d_normed, norm_gain)


def summed(parts, copies):
    _, count, rows = parts.shape

    def kernel(parts_r, o_ref):
        o_ref[...] = jnp.broadcast_to(jnp.sum(parts_r[...], axis=0)[None], (copies, count, rows))

    return pl.pallas_call(
        kernel,
        out_shape=jax.ShapeDtypeStruct((copies, count, rows), f32),
        compiler_params=pltpu.CompilerParams(vmem_limit_bytes=GRANT),
        cost_estimate=pl.CostEstimate(
            flops=parts.size, bytes_accessed=4 * (parts.size + copies * count * rows), transcendentals=0
        ),
    )(parts)


def products(own_weight, pair_weight, inputs, picks, core, slot_rows=None, width=None):
    features, cols = own_weight.shape[-2:]
    half, groups, each = Y // 2, 2, 2
    rows = inputs[0].shape[1] if slot_rows else inputs[1].shape[0]

    def fetches(pick, weights, blocks, sems):
        copies = []
        for n in range(groups * each):
            from_y = pl.ds(n // each * half, half)
            copies.append(
                [
                    pltpu.make_async_copy(
                        weight.at[pick[n], from_y, pick[groups * each]],
                        blocks.at[m, n],
                        sems.at[m, n],
                    )
                    for m, weight in enumerate(weights)
                ]
            )
        for pair in copies:
            for copy in pair:
                copy.start()
        return copies

    def block_product(copies, blocks, gradients, n):
        total = 0.0
        for m, copy in enumerate(copies[n]):
            copy.wait()
            w = blocks[m, n].reshape(half * features, cols)
            total = total + jnp.dot(w, gradients[m][...], preferred_element_type=f32)
        return total.astype(bf16).reshape(half, features, rows)

    def begun(source, target, sem):
        copy = pltpu.make_async_copy(source, target, sem)
        copy.start()
        return copy

    def first(
        pick, own_w, pair_w, sums, own_r, own_g, packed, gain, out_a, out_b, own_d, pair_d, normed,
        blocks, sems, own_v, pair_v, normed_v, out_v, more,
    ):
        copies = fetches(pick, (own_w, pair_w), blocks, sems)
        total = jnp.sum(sums[...], axis=0)
        full = jnp.concatenate([total, jnp.zeros((LANES - total.shape[0], rows), f32)], axis=0)
        columns = full.T
        inverse = lax.rsqrt(columns[:, 0:1] / width + epsilon)
        cross_mean = columns[:, 1:2] / width

        def gradient(wide, grad):
            d_rows = inverse * (grad - wide * inverse * inverse * cross_mean)
            return d_rows.T.astype(bf16)

        wide = own_r[...].astype(f32)
        own_v[...] = gradient(wide, own_g[...])
        pair_v[...] = gradient(packed[1], packed[0])
        leaving = [begun(own_v, own_d, more.at[0]), begun(pair_v, pair_d, more.at[1])]
        for n in range(groups * each):
            out_v[n] = block_product(copies, blocks, (own_v, pair_v), n)
            out = (out_a, out_b)[n // each]
            leaving.append(begun(out_v.at[n], out.at[n % each], more.at[3 + n]))
        normed_v[...] = (wide * inverse * gain[...]).astype(bf16)
        leaving.append(begun(normed_v, normed, more.at[2]))
        for copy in leaving:
            copy.wait()

    def second(
        pick, own_w, pair_w, own_d, pair_d, normed, slot, out_a, out_b, outgoing,
        blocks, sems, own_v, pair_v, normed_v, out_v, more,
    ):
        arriving = [begun(own_d, own_v, more.at[0]), begun(pair_d, pair_v, more.at[1])]
        arriving.append(begun(normed, normed_v, more.at[2]))
        copies = fetches(pick, (own_w, pair_w), blocks, sems)
        sender = lax.broadcasted_iota(jnp.int32, (slot_rows, rows), 0) == slot[...]
        sender = jnp.where(sender, 1.0, 0.0).astype(bf16)
        for copy in arriving:
            copy.wait()
        out_v[...] = jnp.dot(sender, normed_v[...], preferred_element_type=f32).astype(bf16)
        leaving = begun(out_v, outgoing, more.at[3])
        for n in range(groups * each):
            out = (out_a, out_b)[n // each]
            out[n % each] = block_product(copies, blocks, (own_v, pair_v), n)
        leaving.wait()

    vmem, hbm = pl.BlockSpec(memory_space=pltpu.VMEM), pl.BlockSpec(memory_space=pltpu.HBM)
    group_shape = (each, half, features, rows)
    if slot_rows:
        out_shape = [jax.ShapeDtypeStruct(group_shape, bf16)] * groups
        out_shape += [pltpu.HBM((slot_rows, cols), bf16)]
        in_specs, out_specs = [hbm] * 3 + [vmem], [vmem] * groups + [hbm]
        held = (slot_rows, cols)
    else:
        out_shape = [pltpu.HBM(group_shape, bf16)] * groups
        out_shape += [pltpu.HBM((cols, rows), bf16)] * 2 + [pltpu.HBM((rows, cols), bf16)]
        in_specs, out_specs = [vmem] * len(inputs), [hbm] * len(out_shape)
        held = (groups * each, half, features, rows)
    return pl.pallas_call(
        second if slot_rows else first,
        in_specs=[pl.BlockSpec(memory_space=pltpu.SMEM), hbm, hbm] + in_specs,
        out_specs=out_specs,
        out_shape=out_shape,
        scratch_shapes=[
            pltpu.VMEM((C, groups * each, half, features, cols), bf16),
            pltpu.SemaphoreType.DMA((C, groups * each)),
            pltpu.VMEM((cols, rows), bf16),
            pltpu.VMEM((cols, rows), bf16),
            pltpu.VMEM((rows, cols), bf16),
            pltpu.VMEM(held, bf16),
            pltpu.SemaphoreType.DMA((3 + groups * each,)),
        ],
        compiler_params=pltpu.CompilerParams(vmem_limit_bytes=GRANT),
        cost_estimate=pl.CostEstimate(
            flops=4 * groups * each * half * features * cols * rows,
            bytes_accessed=2 * groups * each * half * features * (2 * cols + rows),
            transcendentals=rows,
        ),
    )(
        jnp.stack([*picks, core]),
        *(stays(weight) for weight in (own_weight, pair_weight)),
        *(stays(value) if slot_rows and value.dtype == bf16 else value for value in inputs),
    )


def finished(over_y, slope):
    rows, cols = slope.shape

    def kernel(parts, slope_r, o_ref):
        total = jnp.sum(parts[...].astype(f32), axis=0)
        o_ref[...] = (total.T * slope_r[...]).astype(bf16)

    return pl.pallas_call(
        kernel,
        out_shape=jax.ShapeDtypeStruct((rows, cols), bf16),
        compiler_params=pltpu.CompilerParams(vmem_limit_bytes=GRANT),
        cost_estimate=pl.CostEstimate(
            flops=6 * rows * cols, bytes_accessed=14 * rows * cols, transcendentals=0
        ),
    )(over_y, slope)


def combined(kept_a, got_a, last_a, kept_b, got_b, last_b):
    half, features, rows = last_a.shape

    def kernel(kept_a, got_a, last_a, kept_b, got_b, last_b, o_ref):
        for at, parts in ((0, (kept_a, got_a, last_a)), (half, (kept_b, got_b, last_b))):
            total = sum(part[...].astype(f32) for part in parts)
            o_ref[pl.ds(at, half)] = total.astype(bf16)

    second = pl.BlockSpec((None, half, features, rows), lambda i: (1, 0, 0, 0))
    whole = pl.BlockSpec((half, features, rows), lambda i: (0, 0, 0))
    return pl.pallas_call(
        kernel,
        grid=(1,),
        in_specs=[second, second, whole] * 2,
        out_specs=pl.BlockSpec((2 * half, features, rows), lambda i: (0, 0, 0)),
        out_shape=jax.ShapeDtypeStruct((2 * half, features, rows), bf16),
        compiler_params=pltpu.CompilerParams(vmem_limit_bytes=GRANT),
        cost_estimate=pl.CostEstimate(
            flops=4 * half * features * rows,
            bytes_accessed=16 * half * features * rows,
            transcendentals=0,
        ),
    )(kept_a, got_a, last_a, kept_b, got_b, last_b)


def swap_pair(value):
    return lax.ppermute(value, "core", [(0, 1), (1, 0)])


def swap_even(value):
    return lax.ppermute(value, "x", [(i, i ^ 1) for i in range(X)])


def swap_odd(value):
    return lax.ppermute(value, "x", [(i, 3 - i) for i in range(X)])


def swap_all(value, axis):
    return lax.all_to_all(value, axis, split_axis=0, concat_axis=0, tiled=True)


def on_device(hidden, proj_weight, proj_bias, tile_pos, text_embed, norm_gain, d_normed):
    rows_dev, model_width = hidden.shape
    local_cols = proj_weight.shape[1]
    tok_dev = text_embed.shape[0]
    groups = lax.axis_size("grp")
    group_index = lax.axis_index("grp")
    core = lax.axis_index("core")
    here = lax.axis_index("x")
    lane_index = (here * Y + lax.axis_index("y")) * C + core
    tiles_dev = rows_dev // TILE
    spread = tok_dev // TILE
    total_tiles = tiles_dev * groups
    capacity = max(2, (tiles_dev + groups - 1) // groups)
    slot_rows = groups * capacity * TILE

    fetch_out, standing, doc_slot = outset(tile_pos, group_index, d_normed, groups, capacity)
    tile_index = jnp.arange(total_tiles, dtype=jnp.int32)
    slot = tile_pos // spread * capacity + standing[0]
    receiver = (doc_slot == jnp.arange(slot_rows, dtype=jnp.int32)[:, None]).astype(bf16)
    row = jnp.arange(rows_dev, dtype=jnp.int32)
    own_tile = (tile_index - group_index * tiles_dev)[:, None] == (row // TILE)[None, :]
    found = slot[:, None] * TILE + (row % TILE)[None, :]
    image_slot = jnp.sum(jnp.where(own_tile, found, 0), axis=0)
    sender = match_table(image_slot, slot_rows).astype(bf16)

    def scattered(table, rows):
        return lax.dot_general(table, rows, (((0,), (0,)), ((), ())), preferred_element_type=f32)

    def exchange(rows):
        split = rows.reshape(groups, capacity * TILE, local_cols)
        return swap_all(split, "grp").reshape(slot_rows, local_cols)

    fetch_in = exchange(fetch_out)

    pair_weight = swap_pair(proj_weight)

    activated = gelu(hidden.astype(f32)).astype(bf16)
    image_rows = jnp.dot(activated, proj_weight, preferred_element_type=f32) + proj_bias
    image_rows = image_rows.astype(bf16)

    image_cot = scattered(sender, fetch_in).astype(bf16)
    image_grad = image_cot.astype(f32) * norm_gain

    gain_row = norm_gain.reshape(1, local_cols)
    copies, packed = row_sums(image_rows, image_grad, text_embed, d_normed, gain_row)
    sums = swap_all(copies, ("x", "core"))
    sums = swap_all(summed(sums, Y), "y")
    pair_image = swap_pair(packed)

    even, odd = here ^ 1, 3 - here
    shape = (X, Y, C, local_cols, local_cols)
    own_weight, pair_weight = proj_weight.reshape(shape), pair_weight.reshape(shape)
    sent_a, sent_b, own_d, pair_d, image_normed = products(
        own_weight,
        pair_weight,
        (sums, image_rows, image_grad, pair_image, gain_row),
        (3 - even, even, odd ^ 1, odd),
        core,
        width=model_width,
    )
    got_a = swap_even(sent_a)
    got_b = swap_odd(sent_b)

    kept_a, kept_b, outgoing = products(
        own_weight,
        pair_weight,
        (own_d, pair_d, image_normed, image_slot.reshape(1, rows_dev)),
        (odd, here, even, here),
        core,
        slot_rows=slot_rows,
    )

    def both(kept, got, index):
        return kept[index].astype(f32) + got[index].astype(f32)

    last_a = swap_odd(both(kept_a, got_a, 0).astype(bf16))
    last_b = swap_even(both(kept_b, got_b, 0).astype(bf16))
    over_x = combined(kept_a, got_a, last_a, kept_b, got_b, last_b)
    over_y = swap_all(over_x, "y")
    own_hidden = lax.dynamic_slice_in_dim(hidden, lane_index * local_cols, local_cols, 1)
    slope = gelu_slope(own_hidden.astype(f32))
    d_hidden = finished(over_y, slope)

    incoming = exchange(outgoing)
    placed = scattered(receiver, incoming).astype(bf16)

    text_sums = jnp.sum(sums[:, 2:], axis=0)
    text_sq, text_cr = text_sums.reshape(2, tok_dev)
    inverse = lax.rsqrt(text_sq / model_width + epsilon)[:, None]
    cross_mean = (text_cr / model_width)[:, None]
    is_image = (doc_slot >= 0).reshape(tok_dev, 1)
    text_wide = text_embed.astype(f32)
    text_grad = d_normed.astype(f32) * norm_gain
    text_normed = (text_wide * inverse * norm_gain).astype(bf16)
    normed = jnp.where(is_image, placed, text_normed)
    d_text = inverse * (text_grad - text_wide * inverse * inverse * cross_mean)
    d_text = jnp.where(is_image, 0.0, d_text).astype(bf16)
    return (normed, d_text, d_hidden)


def solution(mesh):
    groups = mesh.shape["grp"]
    fine = Mesh(mesh.devices.reshape(groups, X, Y, C), ("grp", "x", "y", "core"))
    tp = ("x", "y", "core")
    in_specs = (
        P("grp", None),
        P(None, tp),
        P(tp),
        P(),
        P("grp", tp),
        P(tp),
        P("grp", tp),
    )
    out_specs = (P("grp", tp), P("grp", tp), P("grp", tp))

    return jax.shard_map(on_device, mesh=fine, in_specs=in_specs, out_specs=out_specs, check_vma=False)
```
